32 devices in a mesh: gx: 4 (over y, x), gy: 8 (over z, core).
Axes of the slice: x: 2, y: 2, z: 4, core: 2. Of those that a mesh axis runs over, the one named last changes fastest.
Arguments:
- cotangent: float32 [128, 512, 128], P('gx', 'gy'), may hold values from -6 to 6
- speed: float32 [3, 128, 512, 128], P(None, 'gx', 'gy'), may hold values from 0.05 to 0.45
- coeff: float32 [3, 128, 512, 128], P(None, 'gx', 'gy'), may hold values from 0.3 to 3
- dirs: int32 [3, 128, 512], P(None, 'gx', 'gy'), may hold values from 0 to 1
Outputs:
- grad: float32 [128, 512, 128], P('gx', 'gy')
The draws below stay inside these ranges and needn't reach their ends.
Inputs may be any that keep to these rules, and one draw needn't show every extreme that they name: `dirs`: 0 means the lower cell of a face is upwind, 1 the upper cell.
All inputs are finite; a program needn't handle non-finite values.
Results may differ from the reference program's by a relative error of at most 0.0003.
Values sent between devices are 32-bit elements; how exact they have to be, the bound alone decides.
A program may use at most 128 MiB of HBM per device.

```python
import math
import jax
import jax.numpy as jnp
from jax import lax

NZ = 128
ITERS = 2
NX = 128
NY = 512


def plant(array, rng, smallest, top_value):
    index_at = [jax.random.randint(jax.random.fold_in(rng, axis), (), 0, length) for axis, length in enumerate(array.shape)]
    main_axis = array.shape.index(max(array.shape))
    next_to = index_at[:main_axis] + [(index_at[main_axis] + 1) % array.shape[main_axis]] + index_at[main_axis + 1:]
    return array.at[tuple(index_at)].set(smallest).at[tuple(next_to)].set(top_value)


def shard_levels(own_key, shape, pieces, smallest, top_value):
    gain = 1.0
    for dim, parts in pieces:
        steps = jax.random.uniform(jax.random.fold_in(jax.random.fold_in(own_key, 6), dim), (parts,), jnp.float32, smallest / len(pieces), top_value / len(pieces))
        gain = gain * jnp.repeat(jnp.exp(steps), shape[dim] // parts).reshape((-1,) + (1,) * (len(shape) - 1 - dim))
    return gain


def scatter_about(rng, dims, width, limit, shards=(), held_as=jnp.bfloat16):
    drawn = width * jax.random.normal(rng, dims, jnp.float32)
    if shards:
        drawn = drawn * shard_levels(rng, dims, shards, -0.22, 0.18)
    return jnp.clip(drawn, -limit, limit).astype(held_as)


def setup_inputs(seed: int = 0) -> dict:
    seeds = jax.random.split(jax.random.key(seed), 5)
    return {
        "cotangent": scatter_about(seeds[0], (NX, NY, NZ), 1.0, 6.0, ((0, 4), (1, 8)), jnp.float32),
        "speed": jnp.clip(jnp.exp(math.log(0.45) - 2.1972245 * jax.random.uniform(seeds[1], (3, NX, NY, NZ), jnp.float32) ** shard_levels(seeds[1], (3, NX, NY, NZ), ((1, 4), (2, 8)), -0.2, 0.2)), 0.05, 0.45),
        "coeff": jnp.clip(jnp.exp(math.log(3.0) - 2.3025851 * jax.random.uniform(seeds[2], (3, NX, NY, NZ), jnp.float32) ** shard_levels(seeds[2], (3, NX, NY, NZ), ((1, 4), (2, 8)), -0.2, 0.2)), 0.3, 3.0),
        "dirs": plant(jax.random.randint(seeds[3], (3, NX, NY), 0, 2), jax.random.fold_in(seeds[3], 1), 0, 1).astype(jnp.int32),
    }


explicit_table = ((0.0, 0.0, 0.0, 0.0), (0.5, 0.0, 0.0, 0.0), (0.25, 0.5, 0.0, 0.0), (0.2, 0.3, 0.5, 0.0))
implicit_table = ((0.0, 0.0, 0.0, 0.0), (0.25, 0.25, 0.0, 0.0), (0.25, 0.25, 0.25, 0.0), (0.15, 0.35, 0.25, 0.25))
section_weights = (0.15, 0.35, 0.25, 0.25)
implicit_diagonal = 0.25
step_length = 1.0


def local_ahead(values, dimension):
    tail = lax.slice_in_dim(values, 1, values.shape[dimension], axis=dimension)
    return jnp.concatenate([tail, jnp.zeros_like(lax.slice_in_dim(values, 0, 1, axis=dimension))], dimension)


def local_behind(values, dimension):
    head = lax.slice_in_dim(values, 0, values.shape[dimension] - 1, axis=dimension)
    return jnp.concatenate([jnp.zeros_like(lax.slice_in_dim(values, 0, 1, axis=dimension)), head], dimension)


def transposed(advected, diffused, velocity, coeff):
    total = jnp.zeros_like(diffused)
    for dimension in range(3):
        flux = coeff[dimension] * (local_ahead(diffused, dimension) - diffused)
        total = total + flux - local_behind(flux, dimension)
        if advected is not None:
            moved = velocity[dimension] * (local_ahead(advected, dimension) - advected)
            upwind_here = velocity[dimension] > 0
            total = total + jnp.where(upwind_here, moved, 0.0)
            total = total + local_behind(jnp.where(upwind_here, 0.0, moved), dimension)
    return total


def solve_section(rhs, velocity, coeff):
    solution = jnp.zeros_like(rhs)
    residual = rhs
    direction = rhs
    norm_now = jnp.sum(residual * residual)
    for iteration in range(ITERS):
        image = direction - implicit_diagonal * step_length * transposed(None, direction, velocity, coeff)
        alpha = norm_now / jnp.sum(direction * image)
        solution = solution + alpha * direction
        residual = residual - alpha * image
        norm_next = jnp.sum(residual * residual)
        direction = residual + (norm_next / norm_now) * direction
        norm_now = norm_next
    return solution


def reference(cotangent, speed, coeff, dirs):
    signs = (1 - 2 * dirs).astype(jnp.float32)
    velocity = speed * signs[..., None]
    section_adjoints = [None, None, None, None]
    for section_index in (3, 2, 1, 0):
        advected = step_length * section_weights[section_index] * cotangent
        diffused = step_length * section_weights[section_index] * cotangent
        for later in range(section_index + 1, 4):
            advected = advected + step_length * explicit_table[later][section_index] * section_adjoints[later]
            diffused = diffused + step_length * implicit_table[later][section_index] * section_adjoints[later]
        source = transposed(advected, diffused, velocity, coeff)
        if section_index > 0:
            section_adjoints[section_index] = solve_section(source, velocity, coeff)
        else:
            section_adjoints[section_index] = source
    return cotangent + section_adjoints[0] + section_adjoints[1] + section_adjoints[2] + section_adjoints[3]
```

```python
import functools

import jax
import jax.numpy as jnp
from jax import lax
from jax.experimental import pallas as pl
from jax.experimental.pallas import tpu as pltpu
from jax.sharding import PartitionSpec as P

explicit_table = (
    (0.0, 0.0, 0.0, 0.0),
    (0.5, 0.0, 0.0, 0.0),
    (0.25, 0.5, 0.0, 0.0),
    (0.2, 0.3, 0.5, 0.0),
)
implicit_table = (
    (0.0, 0.0, 0.0, 0.0),
    (0.25, 0.25, 0.0, 0.0),
    (0.25, 0.25, 0.25, 0.0),
    (0.15, 0.35, 0.25, 0.25),
)
section_weights = (0.15, 0.35, 0.25, 0.25)
implicit_diagonal = 0.25

MESH = pl.DeviceIdType.MESH
PAD = 8


def kernel(
    gx, gy, cot_hbm, speed_hbm, coeff_hbm, dirs_ref, out_ref,
    fields, mixes, cx, cy, cz, czm, px, py, pz, mx, my, mz, gdiag, fdiag,
    ysend, yrecv, landed, red_y, red_x, load_sem, send_sem, recv_sem, rys, ryr, rxs, rxr,
):
    nx, ny, nz = out_ref.shape
    me_x, me_y = lax.axis_index("gx"), lax.axis_index("gy")
    own = pl.ds(PAD, ny)
    up = pl.ds(PAD + 1, ny)
    down = pl.ds(PAD - 1, ny)
    lane = lax.broadcasted_iota(jnp.int32, (ny, nz), 1)
    last_lane = lane == nz - 1

    def ahead_z(v):
        return pltpu.roll(v, nz - 1, 1)

    def behind_z(v):
        return pltpu.roll(v, 1, 1)

    loads = [
        pltpu.make_async_copy(src, dst, load_sem.at[k])
        for k, (src, dst) in enumerate((
            (speed_hbm.at[0], mx.at[pl.ds(1, nx)]),
            (speed_hbm.at[1], my.at[:, own]),
            (speed_hbm.at[2], mz),
            (coeff_hbm.at[0], cx.at[pl.ds(1, nx)]),
            (coeff_hbm.at[1], cy.at[:, own]),
            (coeff_hbm.at[2], cz),
            (cot_hbm, fields.at[0, pl.ds(1, nx), own]),
        ))
    ]
    for load in loads:
        load.start()

    plane = jnp.zeros((ny, nz), jnp.float32)
    for k in range(7):
        fields[k, 0, own] = plane
        fields[k, nx + 1, own] = plane
    cx[0] = plane
    mx[0] = plane
    landed[0] = plane
    landed[1] = plane
    yrecv[...] = jnp.zeros_like(yrecv)

    def zero_rows(x, carry):
        cy[x, pl.ds(0, PAD)] = jnp.zeros((PAD, nz), jnp.float32)
        my[x, pl.ds(0, PAD)] = jnp.zeros((PAD, nz), jnp.float32)
        return carry

    lax.fori_loop(0, nx, zero_rows, 0)

    barrier = pltpu.get_barrier_semaphore()
    for off in range(1, gx):
        pl.semaphore_signal(barrier, inc=1, device_id={"gx": lax.rem(me_x + off, gx)}, device_id_type=MESH)
    for off in range(1, gy):
        pl.semaphore_signal(barrier, inc=1, device_id={"gy": lax.rem(me_y + off, gy)}, device_id_type=MESH)
    pl.semaphore_wait(barrier, gx + gy - 2)

    def x_down(tag, src, dst):
        return pltpu.make_async_remote_copy(
            src, dst, send_sem.at[tag, 0], recv_sem.at[tag, 0],
            device_id={"gx": lax.rem(me_x + gx - 1, gx)}, device_id_type=MESH)

    def x_up(tag, src, dst):
        return pltpu.make_async_remote_copy(
            src, dst, send_sem.at[tag, 1], recv_sem.at[tag, 1],
            device_id={"gx": lax.rem(me_x + 1, gx)}, device_id_type=MESH)

    def y_down(tag):
        return pltpu.make_async_remote_copy(
            ysend.at[tag, 0], yrecv.at[tag, 1], send_sem.at[tag, 2], recv_sem.at[tag, 2],
            device_id={"gy": lax.rem(me_y + gy - 1, gy)}, device_id_type=MESH)

    def y_up(tag):
        return pltpu.make_async_remote_copy(
            ysend.at[tag, 1], yrecv.at[tag, 0], send_sem.at[tag, 3], recv_sem.at[tag, 3],
            device_id={"gy": lax.rem(me_y + 1, gy)}, device_id_type=MESH)

    def copies(tag):
        field = fields.at[tag]
        return (
            x_down(tag, field.at[1, own], field.at[nx + 1, own]),
            x_up(tag, field.at[nx, own], field.at[0, own]),
            y_down(tag),
            y_up(tag),
        )

    not_low = (me_x > 0, me_y > 0)
    not_high = (me_x < gx - 1, me_y < gy - 1)

    def start(tag):
        xd, xu, yd, yu = copies(tag)
        pl.when(not_low[0])(xd.start)
        pl.when(not_high[0])(xu.start)
        pl.when(not_low[1])(yd.start)
        pl.when(not_high[1])(yu.start)

    def finish(tag):
        xd, xu, yd, yu = copies(tag)
        pl.when(not_high[0])(xd.wait_recv)
        pl.when(not_low[0])(xu.wait_recv)
        pl.when(not_high[1])(yd.wait_recv)
        pl.when(not_low[1])(yu.wait_recv)
        pl.when(not_low[0])(xd.wait_send)
        pl.when(not_high[0])(xu.wait_send)
        pl.when(not_low[1])(yd.wait_send)
        pl.when(not_high[1])(yu.wait_send)
        for x in range(nx):
            fields[tag, 1 + x, pl.ds(PAD - 1, 1)] = yrecv[tag, 0, pl.ds(x, 1)]
            fields[tag, 1 + x, pl.ds(PAD + ny, 1)] = yrecv[tag, 1, pl.ds(x, 1)]

    for load in loads:
        load.wait()

    dirs = [dirs_ref[d].astype(jnp.float32).T for d in range(3)]

    def prepare(x, carry):
        column = (lax.broadcasted_iota(jnp.int32, (nx, nz), 0) == x).astype(jnp.float32)
        upper = [
            jnp.dot(dirs[d], column, preferred_element_type=jnp.float32) > 0.5 for d in range(3)
        ]
        total = jnp.zeros((ny, nz), jnp.float32)
        s = mx[x + 1]
        total += mx[x]
        m = jnp.where(upper[0], s, 0.0)
        mx[x + 1] = m
        px[x] = s - m
        total += s - m
        s = my[x, own]
        m = jnp.where(upper[1], s, 0.0)
        my[x, own] = m
        py[x] = s - m
        total += s - m
        total += my[x, down]
        s = mz[x]
        m = jnp.where(upper[2], s, 0.0)
        p = s - m
        total += p
        m = jnp.where(last_lane, 0.0, m)
        total += behind_z(m)
        mz[x] = m
        pz[x] = jnp.where(last_lane, 0.0, p)
        fdiag[x] = total
        c = cz[x]
        m = jnp.where(last_lane, 0.0, c)
        czm[x] = m
        gdiag[x] = cx[x + 1] + cx[x] + cy[x, own] + cy[x, down] + c + behind_z(m)
        at = pl.ds(x, 1)
        ysend[0, 0, at] = fields[0, x + 1, pl.ds(PAD, 1)]
        ysend[0, 1, at] = fields[0, x + 1, pl.ds(PAD + ny - 1, 1)]
        ysend[7, 1, at] = cy[x, pl.ds(PAD + ny - 1, 1)]
        ysend[8, 1, at] = my[x, pl.ds(PAD + ny - 1, 1)]
        return carry

    lax.fori_loop(0, nx, prepare, 0)

    start(0)
    statics = (
        (x_up(7, cx.at[nx], landed.at[0]), y_up(7)),
        (x_up(8, mx.at[nx], landed.at[1]), y_up(8)),
    )
    for xu, yu in statics:
        pl.when(not_high[0])(xu.start)
        pl.when(not_high[1])(yu.start)
    for xu, yu in statics:
        pl.when(not_low[0])(xu.wait_recv)
        pl.when(not_low[1])(yu.wait_recv)
        pl.when(not_high[0])(xu.wait_send)
        pl.when(not_high[1])(yu.wait_send)
    finish(0)
    cx[0] = landed[0]
    mx[0] = landed[1]
    gdiag[0] += cx[0]
    fdiag[0] += mx[0]
    first = pl.ds(0, 1)
    for x in range(nx):
        row = yrecv[7, 0, pl.ds(x, 1)]
        cy[x, pl.ds(PAD - 1, 1)] = row
        gdiag[x, first] += row
        row = yrecv[8, 0, pl.ds(x, 1)]
        my[x, pl.ds(PAD - 1, 1)] = row
        fdiag[x, first] += row

    def spread(ref, x):
        v = ref[x + 1, own]
        total = cx[x + 1] * ref[x + 2, own] + cx[x] * ref[x, own]
        total += cy[x, own] * ref[x + 1, up] + cy[x, down] * ref[x + 1, down]
        c = czm[x]
        total += c * ahead_z(v) + behind_z(c * v)
        return v, total - gdiag[x] * v

    def carried(ref, x):
        v = ref[x + 1, own]
        total = px[x] * ref[x + 2, own] + mx[x] * ref[x, own]
        total += py[x] * ref[x + 1, up] + my[x, down] * ref[x + 1, down]
        total += pz[x] * ahead_z(v) + behind_z(mz[x] * v)
        return total - fdiag[x] * v

    def fold(v):
        return jnp.sum(v.reshape(ny // 8, 8, nz), axis=0)

    nothing = jnp.zeros((8, nz), jnp.float32)

    def keep(tag, x, v):
        fields[tag, x + 1, own] = v
        ysend[tag, 0, pl.ds(x, 1)] = v[:1]
        ysend[tag, 1, pl.ds(x, 1)] = v[ny - 1:]

    def reduced(step, sums):
        rows = [jnp.sum(s, axis=0, keepdims=True) for s in sums]
        red_y[step, me_y] = jnp.concatenate(rows + [jnp.zeros((4, nz), jnp.float32)], axis=0)

        def across(slots, axis, me, count, send, recv):
            out = [
                pltpu.make_async_remote_copy(
                    slots.at[step, me], slots.at[step, me], send.at[step, off], recv.at[step, me],
                    device_id={axis: lax.rem(me + off, count)}, device_id_type=MESH)
                for off in range(1, count)
            ]
            for copy in out:
                copy.start()
            for off in range(1, count):
                peer = lax.rem(me + off, count)
                pltpu.make_async_remote_copy(
                    slots.at[step, peer], slots.at[step, peer], send.at[step, off], recv.at[step, peer],
                    device_id={axis: peer}, device_id_type=MESH).wait_recv()
            total = slots[step, 0]
            for k in range(1, count):
                total = total + slots[step, k]
            for copy in out:
                copy.wait_send()
            return total

        red_x[step, me_x] = across(red_y, "gy", me_y, gy, rys, ryr)
        total = across(red_x, "gx", me_x, gx, rxs, rxr)
        total = jnp.broadcast_to(jnp.sum(total, axis=1, keepdims=True), (8, nz))
        return [total[k:k + 1] for k in range(4)]

    for step, section in enumerate((3, 2, 1, 0)):
        weight = section_weights[section]
        if step:
            def mix(x, carry):
                base = weight * fields[0, x]
                adv, dif = base, base
                for k in range(step):
                    later = 3 - k
                    nu = fields[4 + k, x]
                    adv = adv + explicit_table[later][section] * nu
                    dif = dif + implicit_table[later][section] * nu
                mixes[0, x] = adv
                mixes[1, x] = dif
                return carry

            lax.fori_loop(0, nx + 2, mix, 0)

        def source(x):
            if step == 0:
                field = fields.at[0]
                return weight * (spread(field, x)[1] + carried(field, x))
            return spread(mixes.at[1], x)[1] + carried(mixes.at[0], x)

        if section == 0:
            def last(x, carry):
                total = fields[0, x + 1, own] + source(x)
                for k in range(3):
                    total = total + fields[4 + k, x + 1, own]
                out_ref[x] = total
                return carry

            lax.fori_loop(0, nx, last, 0)
            break

        r_tag, w_tag = 1 + step, 4 + step

        def first_pass(x, m0):
            r = source(x)
            keep(r_tag, x, r)
            return m0 + fold(r * r)

        m0 = lax.fori_loop(0, nx, first_pass, nothing)
        start(r_tag)
        finish(r_tag)

        def second_pass(x, sums):
            m1, m2 = sums
            r, d = spread(fields.at[r_tag], x)
            w = r - implicit_diagonal * d
            keep(w_tag, x, w)
            return m1 + fold(r * w), m2 + fold(w * w)

        m1, m2 = lax.fori_loop(0, nx, second_pass, (nothing, nothing))
        start(w_tag)
        finish(w_tag)

        def third_pass(x, m3):
            ref = fields.at[w_tag]
            w = ref[x + 1, own]
            jump_x = ref[x + 2, own] - w
            jump_y = ref[x + 1, up] - w
            jump_z = jnp.where(last_lane, 0.0, ahead_z(w)) - w
            total = cx[x + 1] * jump_x * jump_x + cy[x, own] * jump_y * jump_y
            total += cz[x] * jump_z * jump_z
            return m3 + fold(implicit_diagonal * total)

        m3 = m2 + lax.fori_loop(0, nx, third_pass, nothing)
        m0, m1, m2, m3 = reduced(step, (m0, m1, m2, m3))
        alpha = m0 / m1
        rr = alpha * alpha * m2 - m0
        ratio = rr / m0
        product = m1 - 2.0 * alpha * m2 + alpha * alpha * m3
        alpha_next = rr / (product - ratio * rr / alpha)
        on_r = alpha + alpha_next * (1.0 + ratio)
        on_w = -alpha_next * alpha

        def combine(x, carry):
            fields[w_tag, x] = on_r * fields[r_tag, x] + on_w * fields[w_tag, x]
            return carry

        lax.fori_loop(0, nx + 2, combine, 0)


def local(gx, gy, cotangent, speed, coeff, dirs):
    nx, ny, nz = cotangent.shape
    f32 = jnp.float32
    rows = ny + 2 * PAD
    plain = pltpu.VMEM((nx, ny, nz), f32)
    dma = pltpu.SemaphoreType.DMA
    anywhere = pl.BlockSpec(memory_space=pl.ANY)
    return pl.pallas_call(
        functools.partial(kernel, gx, gy),
        out_shape=jax.ShapeDtypeStruct((nx, ny, nz), f32),
        in_specs=[anywhere, anywhere, anywhere, pl.BlockSpec(memory_space=pltpu.VMEM)],
        out_specs=pl.BlockSpec(memory_space=pltpu.VMEM),
        scratch_shapes=[
            pltpu.VMEM((7, nx + 2, rows, nz), f32),
            pltpu.VMEM((2, nx + 2, rows, nz), f32),
            pltpu.VMEM((nx + 1, ny, nz), f32),
            pltpu.VMEM((nx, rows, nz), f32),
            plain, plain,
            plain, plain, plain,
            pltpu.VMEM((nx + 1, ny, nz), f32),
            pltpu.VMEM((nx, rows, nz), f32),
            plain,
            plain, plain,
            pltpu.VMEM((9, 2, nx, nz), f32),
            pltpu.VMEM((9, 2, nx, nz), f32),
            pltpu.VMEM((2, ny, nz), f32),
            pltpu.VMEM((3, gy, 8, nz), f32),
            pltpu.VMEM((3, gx, 8, nz), f32),
            dma((7,)), dma((9, 4)), dma((9, 4)),
            dma((3, gy)), dma((3, gy)), dma((3, gx)), dma((3, gx)),
        ],
        compiler_params=pltpu.CompilerParams(
            collective_id=0, has_side_effects=True, vmem_limit_bytes=60 * 1024 * 1024
        ),
    )(cotangent, speed, coeff, dirs)


def solution(mesh):
    return jax.shard_map(
        functools.partial(local, mesh.shape["gx"], mesh.shape["gy"]),
        mesh=mesh,
        in_specs=(
            P("gx", "gy", None),
            P(None, "gx", "gy", None),
            P(None, "gx", "gy", None),
            P(None, "gx", "gy"),
        ),
        out_specs=P("gx", "gy", None),
        check_vma=False,
    )
```

```python
import functools

import jax
import jax.numpy as jnp
from jax import lax
from jax.experimental import pallas as pl
from jax.experimental.pallas import tpu as pltpu
from jax.sharding import PartitionSpec as P

explicit_table = (
    (0.0, 0.0, 0.0, 0.0),
    (0.5, 0.0, 0.0, 0.0),
    (0.25, 0.5, 0.0, 0.0),
    (0.2, 0.3, 0.5, 0.0),
)
implicit_table = (
    (0.0, 0.0, 0.0, 0.0),
    (0.25, 0.25, 0.0, 0.0),
    (0.25, 0.25, 0.25, 0.0),
    (0.15, 0.35, 0.25, 0.25),
)
section_weights = (0.15, 0.35, 0.25, 0.25)
implicit_diagonal = 0.25

MESH = pl.DeviceIdType.MESH
PAD = 8


def kernel(
    gx, gy, cot_hbm, speed_hbm, coeff_hbm, dirs_ref, out_ref,
    fields, fr, fw, dw, base, cx, cy, cz, czm, px, py, pz, mx, my, mz, gdiag, fdiag,
    ysend, yrecv, landed, stage, red_y, red_x, load_sem, send_sem, recv_sem, rys, ryr, rxs, rxr,
):
    nx, ny, nz = out_ref.shape
    me_x, me_y = lax.axis_index("gx"), lax.axis_index("gy")
    own = pl.ds(PAD, ny)
    up = pl.ds(PAD + 1, ny)
    down = pl.ds(PAD - 1, ny)
    lane = lax.broadcasted_iota(jnp.int32, (ny, nz), 1)
    last_lane = lane == nz - 1

    def ahead_z(v):
        return pltpu.roll(v, nz - 1, 1)

    def behind_z(v):
        return pltpu.roll(v, 1, 1)

    loads = [
        pltpu.make_async_copy(src, dst, load_sem.at[k])
        for k, (src, dst) in enumerate((
            (speed_hbm.at[0], mx.at[pl.ds(1, nx)]),
            (speed_hbm.at[1], my.at[:, own]),
            (speed_hbm.at[2], mz),
            (coeff_hbm.at[0], cx.at[pl.ds(1, nx)]),
            (coeff_hbm.at[1], cy.at[:, own]),
            (coeff_hbm.at[2], cz),
            (cot_hbm, fields.at[0, pl.ds(1, nx), own]),
        ))
    ]
    for load in loads:
        load.start()

    plane = jnp.zeros((ny, nz), jnp.float32)
    for k in range(7):
        fields[k, 0, own] = plane
        fields[k, nx + 1, own] = plane
    cx[0] = plane
    mx[0] = plane
    landed[0] = plane
    landed[1] = plane
    yrecv[...] = jnp.zeros_like(yrecv)

    def zero_rows(x, carry):
        cy[x, pl.ds(0, PAD)] = jnp.zeros((PAD, nz), jnp.float32)
        my[x, pl.ds(0, PAD)] = jnp.zeros((PAD, nz), jnp.float32)
        for k in range(1, 7):
            fields[k, x + 1, pl.ds(0, PAD)] = jnp.zeros((PAD, nz), jnp.float32)
            fields[k, x + 1, pl.ds(PAD + ny, PAD)] = jnp.zeros((PAD, nz), jnp.float32)
        return carry

    lax.fori_loop(0, nx, zero_rows, 0)

    barrier = pltpu.get_barrier_semaphore()
    for off in range(1, gx):
        pl.semaphore_signal(barrier, inc=1, device_id={"gx": lax.rem(me_x + off, gx)}, device_id_type=MESH)
    for off in range(1, gy):
        pl.semaphore_signal(barrier, inc=1, device_id={"gy": lax.rem(me_y + off, gy)}, device_id_type=MESH)
    pl.semaphore_wait(barrier, gx + gy - 2)

    def x_down(tag, src, dst):
        return pltpu.make_async_remote_copy(
            src, dst, send_sem.at[tag, 0], recv_sem.at[tag, 0],
            device_id={"gx": lax.rem(me_x + gx - 1, gx)}, device_id_type=MESH)

    def x_up(tag, src, dst):
        return pltpu.make_async_remote_copy(
            src, dst, send_sem.at[tag, 1], recv_sem.at[tag, 1],
            device_id={"gx": lax.rem(me_x + 1, gx)}, device_id_type=MESH)

    def y_down(tag):
        return pltpu.make_async_remote_copy(
            ysend.at[tag, 0], yrecv.at[tag, 1], send_sem.at[tag, 2], recv_sem.at[tag, 2],
            device_id={"gy": lax.rem(me_y + gy - 1, gy)}, device_id_type=MESH)

    def y_up(tag):
        return pltpu.make_async_remote_copy(
            ysend.at[tag, 1], yrecv.at[tag, 0], send_sem.at[tag, 3], recv_sem.at[tag, 3],
            device_id={"gy": lax.rem(me_y + 1, gy)}, device_id_type=MESH)

    def copies(tag):
        field = fields.at[tag]
        return (
            x_down(tag, field.at[1, own], field.at[nx + 1, own]),
            x_up(tag, field.at[nx, own], field.at[0, own]),
            y_down(tag),
            y_up(tag),
        )

    low_x, low_y = me_x > 0, me_y > 0
    high_x, high_y = me_x < gx - 1, me_y < gy - 1

    def start_x(tag):
        xd, xu, _, _ = copies(tag)
        pl.when(low_x)(xd.start)
        pl.when(high_x)(xu.start)

    def start_y(tag):
        _, _, yd, yu = copies(tag)
        pl.when(low_y)(yd.start)
        pl.when(high_y)(yu.start)

    def arrive(tag):
        xd, xu, yd, yu = copies(tag)
        pl.when(high_y)(yd.wait_recv)
        pl.when(low_y)(yu.wait_recv)
        pl.when(high_x)(xd.wait_recv)
        pl.when(low_x)(xu.wait_recv)

    def sent(tag):
        xd, xu, yd, yu = copies(tag)
        pl.when(low_x)(xd.wait_send)
        pl.when(high_x)(xu.wait_send)
        pl.when(low_y)(yd.wait_send)
        pl.when(high_y)(yu.wait_send)

    def unpack(tag):
        for x in range(nx):
            fields[tag, 1 + x, pl.ds(PAD - 1, 1)] = yrecv[tag, 0, pl.ds(x, 1)]
            fields[tag, 1 + x, pl.ds(PAD + ny, 1)] = yrecv[tag, 1, pl.ds(x, 1)]

    for load in loads:
        load.wait()

    for x in range(nx):
        at = pl.ds(x, 1)
        ysend[0, 0, at] = fields[0, x + 1, pl.ds(PAD, 1)]
        ysend[0, 1, at] = fields[0, x + 1, pl.ds(PAD + ny - 1, 1)]
        ysend[7, 1, at] = cy[x, pl.ds(PAD + ny - 1, 1)]
        ysend[8, 1, at] = my[x, pl.ds(PAD + ny - 1, 1)]
    dirs = [dirs_ref[d].astype(jnp.float32).T for d in range(3)]
    edge = jnp.broadcast_to(dirs_ref[1][:, ny - 1:], (nx, nz))
    ysend[8, 1] = jnp.where(edge > 0, ysend[8, 1], 0.0)

    def upper(d, x):
        column = (lax.broadcasted_iota(jnp.int32, (nx, nz), 0) == x).astype(jnp.float32)
        return jnp.dot(dirs[d], column, preferred_element_type=jnp.float32) > 0.5

    stage[...] = jnp.where(upper(0, nx - 1), mx[nx], 0.0)
    start_x(0)
    start_y(0)
    statics = (
        (x_up(7, cx.at[nx], landed.at[0]), y_up(7)),
        (x_up(8, stage, landed.at[1]), y_up(8)),
    )
    for xu, yu in statics:
        pl.when(high_x)(xu.start)
        pl.when(high_y)(yu.start)

    def prepare(x, carry):
        total = mx[x]
        s = mx[x + 1]
        m = jnp.where(upper(0, x), s, 0.0)
        mx[x + 1] = m
        px[x] = s - m
        total += s - m
        s = my[x, own]
        m = jnp.where(upper(1, x), s, 0.0)
        my[x, own] = m
        py[x] = s - m
        total += s - m
        total += my[x, down]
        s = mz[x]
        m = jnp.where(upper(2, x), s, 0.0)
        p = s - m
        total += p
        m = jnp.where(last_lane, 0.0, m)
        total += behind_z(m)
        mz[x] = m
        pz[x] = jnp.where(last_lane, 0.0, p)
        fdiag[x] = total
        c = cz[x]
        m = jnp.where(last_lane, 0.0, c)
        czm[x] = m
        gdiag[x] = cx[x + 1] + cx[x] + cy[x, own] + cy[x, down] + c + behind_z(m)
        return carry

    lax.fori_loop(0, nx, prepare, 0)

    arrive(0)
    for xu, yu in statics:
        pl.when(low_x)(xu.wait_recv)
        pl.when(low_y)(yu.wait_recv)
    unpack(0)
    cx[0] = landed[0]
    mx[0] = landed[1]
    gdiag[0] += cx[0]
    fdiag[0] += mx[0]
    first = pl.ds(0, 1)
    for x in range(nx):
        row = yrecv[7, 0, pl.ds(x, 1)]
        cy[x, pl.ds(PAD - 1, 1)] = row
        gdiag[x, first] += row
        row = yrecv[8, 0, pl.ds(x, 1)]
        my[x, pl.ds(PAD - 1, 1)] = row
        fdiag[x, first] += row

    def spread(ref, x):
        v = ref[x + 1, own]
        total = cx[x + 1] * ref[x + 2, own] + cx[x] * ref[x, own]
        total += cy[x, own] * ref[x + 1, up] + cy[x, down] * ref[x + 1, down]
        c = czm[x]
        total += c * ahead_z(v) + behind_z(c * v)
        return v, total - gdiag[x] * v

    def carried(ref, x):
        v = ref[x + 1, own]
        total = px[x] * ref[x + 2, own] + mx[x] * ref[x, own]
        total += py[x] * ref[x + 1, up] + my[x, down] * ref[x + 1, down]
        total += pz[x] * ahead_z(v) + behind_z(mz[x] * v)
        return total - fdiag[x] * v

    def fold(v):
        return jnp.sum(v.reshape(v.shape[0] // 8, 8, nz), axis=0)

    nothing = jnp.zeros((8, nz), jnp.float32)

    def keep(tag, x, v):
        fields[tag, x + 1, own] = v
        ysend[tag, 0, pl.ds(x, 1)] = v[:1]
        ysend[tag, 1, pl.ds(x, 1)] = v[ny - 1:]

    def across(step, slots, axis, me, count, send, recv):
        out = [
            pltpu.make_async_remote_copy(
                slots.at[step, me], slots.at[step, me], send.at[step, off], recv.at[step, me],
                device_id={axis: lax.rem(me + off, count)}, device_id_type=MESH)
            for off in range(1, count)
        ]
        for copy in out:
            copy.start()

        def result():
            for off in range(1, count):
                peer = lax.rem(me + off, count)
                pltpu.make_async_remote_copy(
                    slots.at[step, peer], slots.at[step, peer], send.at[step, off], recv.at[step, peer],
                    device_id={axis: peer}, device_id_type=MESH).wait_recv()
            total = slots[step, 0]
            for k in range(1, count):
                total = total + slots[step, k]
            return total

        return out, result

    row_x = lax.broadcasted_iota(jnp.int32, (nx, nz), 0)
    between = jnp.logical_and(row_x > 0, row_x < nx - 1)
    pending = []
    for step, section in enumerate((3, 2, 1)):
        r_tag, w_tag = 1 + step, 4 + step
        r_ref, w_ref = fields.at[r_tag], fields.at[w_tag]

        def first_pass(x, m0):
            if step == 0:
                c_ref = fields.at[0]
                r = section_weights[3] * (spread(c_ref, x)[1] + carried(c_ref, x))
            else:
                r = following(x)
            keep(r_tag, x, r)
            return m0 + fold(r * r)

        m0 = first_pass(nx - 1, first_pass(0, nothing))
        start_x(r_tag)
        m0 = lax.fori_loop(1, nx - 1, first_pass, m0)
        start_y(r_tag)

        def second_pass(x, sums):
            m1, m2 = sums
            r, d = spread(r_ref, x)
            w = r - implicit_diagonal * d
            keep(w_tag, x, w)
            return m1 + fold(r * w), m2 + fold(w * w)

        sums = lax.fori_loop(1, nx - 1, second_pass, (nothing, nothing))
        arrive(r_tag)
        unpack(r_tag)
        m1, m2 = second_pass(nx - 1, second_pass(0, sums))
        start_x(w_tag)
        for side, face in ((0, yrecv[7, 0]), (1, ysend[7, 1])):
            change = jnp.where(between, -implicit_diagonal * face * yrecv[r_tag, side], 0.0)
            w = ysend[w_tag, side]
            ysend[w_tag, side] = w + change
            m1 += fold(ysend[r_tag, side] * change)
            m2 += fold((2.0 * w + change) * change)
        start_y(w_tag)
        for x in range(1, nx - 1):
            fields[w_tag, 1 + x, pl.ds(PAD, 1)] = ysend[w_tag, 0, pl.ds(x, 1)]
            fields[w_tag, 1 + x, pl.ds(PAD + ny - 1, 1)] = ysend[w_tag, 1, pl.ds(x, 1)]

        def third_pass(x, m3):
            w = w_ref[x + 1, own]
            jump_x = w_ref[x + 2, own] - w
            jump_y = w_ref[x + 1, up] - w
            jump_z = jnp.where(last_lane, 0.0, ahead_z(w)) - w
            total = cx[x + 1] * jump_x * jump_x + cy[x, own] * jump_y * jump_y
            total += cz[x] * jump_z * jump_z
            return m3 + fold(total)

        m3 = lax.fori_loop(0, nx - 1, third_pass, nothing)

        def carry_r(x, carry):
            fr[step, x] = carried(r_ref, x)
            return carry

        lax.fori_loop(0, nx, carry_r, 0)
        arrive(w_tag)
        m3 = third_pass(nx - 1, m3)
        above = yrecv[w_tag, 1]
        m3 += fold(ysend[7, 1] * above * (above - 2.0 * ysend[w_tag, 1]))
        m3 = m2 + implicit_diagonal * m3
        rows = [jnp.sum(m, axis=0, keepdims=True) for m in (m0, m1, m2, m3)]
        red_y[step, me_y] = jnp.concatenate(rows + [jnp.zeros((4, nz), jnp.float32)], axis=0)
        out, result = across(step, red_y, "gy", me_y, gy, rys, ryr)
        pending += out
        unpack(w_tag)

        def carry_w(x, carry):
            fw[step, x] = carried(w_ref, x)
            dw[step, x] = spread(w_ref, x)[1]
            return carry

        lax.fori_loop(0, nx, carry_w, 0)
        red_x[step, me_x] = result()
        out, result = across(step, red_x, "gx", me_x, gx, rxs, rxr)
        pending += out

        target = section - 1
        share = section_weights[target] / section_weights[3]

        def gather(x, carry):
            total = share * fields[1, x + 1, own]
            for k in range(step):
                total += explicit_table[3 - k][target] * fr[k, x] + implicit_table[3 - k][target] * dw[k, x]
            if target == 0:
                total += fields[0, x + 1, own]
                for k in range(step):
                    on_r, on_w = weights[k]
                    total += on_r * fields[1 + k, x + 1, own] + on_w * fields[4 + k, x + 1, own]
            base[x] = total
            return carry

        if step == 0:
            weights = []
        lax.fori_loop(0, nx, gather, 0)

        total = result()
        total = jnp.broadcast_to(jnp.sum(total, axis=1, keepdims=True), (8, nz))
        m0, m1, m2, m3 = [total[k:k + 1] for k in range(4)]
        alpha = m0 / m1
        rr = alpha * alpha * m2 - m0
        ratio = rr / m0
        product = m1 - 2.0 * alpha * m2 + alpha * alpha * m3
        alpha_next = rr / (product - ratio * rr / alpha)
        on_r = alpha + alpha_next * (1.0 + ratio)
        on_w = -alpha_next * alpha
        weights.append((on_r, on_w))

        def following(x, step=step, section=section, target=target, on_r=on_r, on_w=on_w):
            r, w = fields[1 + step, x + 1, own], fields[4 + step, x + 1, own]
            advected = on_r * fr[step, x] + on_w * fw[step, x]
            diffused = (on_r / implicit_diagonal) * (r - w) + on_w * dw[step, x]
            total = base[x]
            total += explicit_table[section][target] * advected
            total += implicit_table[section][target] * diffused
            if target == 0:
                return total + on_r * r + on_w * w
            fr[step, x] = advected
            dw[step, x] = diffused
            return total

    def last(x, carry):
        out_ref[x] = following(x)
        return carry

    lax.fori_loop(0, nx, last, 0)
    for xu, yu in statics:
        pl.when(high_x)(xu.wait_send)
        pl.when(high_y)(yu.wait_send)
    for tag in range(7):
        sent(tag)
    for copy in pending:
        copy.wait_send()


def local(gx, gy, cotangent, speed, coeff, dirs):
    nx, ny, nz = cotangent.shape
    f32 = jnp.float32
    rows = ny + 2 * PAD
    plain = pltpu.VMEM((nx, ny, nz), f32)
    dma = pltpu.SemaphoreType.DMA
    anywhere = pl.BlockSpec(memory_space=pl.ANY)
    return pl.pallas_call(
        functools.partial(kernel, gx, gy),
        out_shape=jax.ShapeDtypeStruct((nx, ny, nz), f32),
        in_specs=[anywhere, anywhere, anywhere, pl.BlockSpec(memory_space=pltpu.VMEM)],
        out_specs=pl.BlockSpec(memory_space=pltpu.VMEM),
        scratch_shapes=[
            pltpu.VMEM((7, nx + 2, rows, nz), f32),
            pltpu.VMEM((3, nx, ny, nz), f32),
            pltpu.VMEM((3, nx, ny, nz), f32),
            pltpu.VMEM((3, nx, ny, nz), f32),
            plain,
            pltpu.VMEM((nx + 1, ny, nz), f32),
            pltpu.VMEM((nx, rows, nz), f32),
            plain, plain,
            plain, plain, plain,
            pltpu.VMEM((nx + 1, ny, nz), f32),
            pltpu.VMEM((nx, rows, nz), f32),
            plain,
            plain, plain,
            pltpu.VMEM((9, 2, nx, nz), f32),
            pltpu.VMEM((9, 2, nx, nz), f32),
            pltpu.VMEM((2, ny, nz), f32),
            pltpu.VMEM((ny, nz), f32),
            pltpu.VMEM((3, gy, 8, nz), f32),
            pltpu.VMEM((3, gx, 8, nz), f32),
            dma((7,)), dma((9, 4)), dma((9, 4)),
            dma((3, gy)), dma((3, gy)), dma((3, gx)), dma((3, gx)),
        ],
        compiler_params=pltpu.CompilerParams(
            collective_id=0, has_side_effects=True, vmem_limit_bytes=60 * 1024 * 1024
        ),
    )(cotangent, speed, coeff, dirs)


def solution(mesh):
    return jax.shard_map(
        functools.partial(local, mesh.shape["gx"], mesh.shape["gy"]),
        mesh=mesh,
        in_specs=(
            P("gx", "gy", None),
            P(None, "gx", "gy", None),
            P(None, "gx", "gy", None),
            P(None, "gx", "gy"),
        ),
        out_specs=P("gx", "gy", None),
        check_vma=False,
    )
```

```python
import functools

import jax
import jax.numpy as jnp
from jax import lax
from jax.experimental import pallas as pl
from jax.experimental.pallas import tpu as pltpu
from jax.sharding import PartitionSpec as P

explicit_table = (
    (0.0, 0.0, 0.0, 0.0),
    (0.5, 0.0, 0.0, 0.0),
    (0.25, 0.5, 0.0, 0.0),
    (0.2, 0.3, 0.5, 0.0),
)
implicit_table = (
    (0.0, 0.0, 0.0, 0.0),
    (0.25, 0.25, 0.0, 0.0),
    (0.25, 0.25, 0.25, 0.0),
    (0.15, 0.35, 0.25, 0.25),
)
section_weights = (0.15, 0.35, 0.25, 0.25)
implicit_diagonal = 0.25

MESH = pl.DeviceIdType.MESH
PAD = 8


GROUP = {"masks": 4, "diagonals": 2, "source": 2, "next": 2, "image": 2, "energy": 4, "carry": 4, "both": 2, "gather": 2}


def grouped(name, low, high, value, store, carry):
    size = GROUP[name]

    def group(planes, carry):
        found = []
        for x in planes:
            carry, kept = value(x, carry)
            found.append(kept)
        for x, kept in zip(planes, found):
            store(x, kept)
        return carry

    turns = (high - low) // size
    carry = lax.fori_loop(
        0, turns, lambda t, c: group([low + t * size + k for k in range(size)], c), carry)
    rest = list(range(low + turns * size, high))
    return group(rest, carry) if rest else carry


def kernel(
    gx, gy, cot_hbm, speed_hbm, coeff_hbm, dirs_ref, out_ref,
    f0, f1, f2, f3, f4, f5, f6, fr0, fr1, fr2, fw0, fw1, fw2, dw0, dw1, dw2, base, cx, cy, cz, czm, px, py, pz, mx, my, mz, gdiag, fdiag,
    ysend, yrecv, landed, stage, red_y, red_x, load_sem, send_sem, recv_sem, rys, ryr, rxs, rxr,
):
    nx, ny, nz = out_ref.shape
    fields = (f0, f1, f2, f3, f4, f5, f6)
    fr, fw, dw = (fr0, fr1, fr2), (fw0, fw1, fw2), (dw0, dw1, dw2)
    me_x, me_y = lax.axis_index("gx"), lax.axis_index("gy")
    own = pl.ds(PAD, ny)
    up = pl.ds(PAD + 1, ny)
    down = pl.ds(PAD - 1, ny)
    lane = lax.broadcasted_iota(jnp.int32, (ny, nz), 1)
    last_lane = lane == nz - 1

    def ahead_z(v):
        return pltpu.roll(v, nz - 1, 1)

    def behind_z(v):
        return pltpu.roll(v, 1, 1)

    loads = [
        pltpu.make_async_copy(src, dst, load_sem.at[k])
        for k, (src, dst) in enumerate((
            (speed_hbm.at[0], px),
            (speed_hbm.at[1], py),
            (speed_hbm.at[2], pz),
            (coeff_hbm.at[0], cx.at[pl.ds(1, nx)]),
            (coeff_hbm.at[1], cy.at[:, own]),
            (coeff_hbm.at[2], cz),
            (cot_hbm, fields[0].at[pl.ds(1, nx), own]),
        ))
    ]
    for load in loads:
        load.start()

    plane = jnp.zeros((ny, nz), jnp.float32)
    for k in range(7):
        fields[k][0, own] = plane
        fields[k][nx + 1, own] = plane
    cx[0] = plane
    mx[0] = plane
    landed[0] = plane
    landed[1] = plane
    yrecv[...] = jnp.zeros_like(yrecv)

    def zero_rows(x, carry):
        cy[x, pl.ds(0, PAD)] = jnp.zeros((PAD, nz), jnp.float32)
        my[x, pl.ds(0, PAD)] = jnp.zeros((PAD, nz), jnp.float32)
        for k in range(1, 7):
            fields[k][x + 1, pl.ds(0, PAD)] = jnp.zeros((PAD, nz), jnp.float32)
            fields[k][x + 1, pl.ds(PAD + ny, PAD)] = jnp.zeros((PAD, nz), jnp.float32)
        return carry

    lax.fori_loop(0, nx, zero_rows, 0)

    barrier = pltpu.get_barrier_semaphore()
    for off in range(1, gx):
        pl.semaphore_signal(barrier, inc=1, device_id={"gx": lax.rem(me_x + off, gx)}, device_id_type=MESH)
    for off in range(1, gy):
        pl.semaphore_signal(barrier, inc=1, device_id={"gy": lax.rem(me_y + off, gy)}, device_id_type=MESH)
    pl.semaphore_wait(barrier, gx + gy - 2)

    def x_down(tag, src, dst):
        return pltpu.make_async_remote_copy(
            src, dst, send_sem.at[tag, 0], recv_sem.at[tag, 0],
            device_id={"gx": lax.rem(me_x + gx - 1, gx)}, device_id_type=MESH)

    def x_up(tag, src, dst):
        return pltpu.make_async_remote_copy(
            src, dst, send_sem.at[tag, 1], recv_sem.at[tag, 1],
            device_id={"gx": lax.rem(me_x + 1, gx)}, device_id_type=MESH)

    def y_down(tag):
        return pltpu.make_async_remote_copy(
            ysend.at[tag, 0], yrecv.at[tag, 1], send_sem.at[tag, 2], recv_sem.at[tag, 2],
            device_id={"gy": lax.rem(me_y + gy - 1, gy)}, device_id_type=MESH)

    def y_up(tag):
        return pltpu.make_async_remote_copy(
            ysend.at[tag, 1], yrecv.at[tag, 0], send_sem.at[tag, 3], recv_sem.at[tag, 3],
            device_id={"gy": lax.rem(me_y + 1, gy)}, device_id_type=MESH)

    def copies(tag):
        field = fields[tag]
        return (
            x_down(tag, field.at[1, own], field.at[nx + 1, own]),
            x_up(tag, field.at[nx, own], field.at[0, own]),
            y_down(tag),
            y_up(tag),
        )

    low_x, low_y = me_x > 0, me_y > 0
    high_x, high_y = me_x < gx - 1, me_y < gy - 1

    def start_x(tag):
        xd, xu, _, _ = copies(tag)
        pl.when(low_x)(xd.start)
        pl.when(high_x)(xu.start)

    def start_y(tag):
        _, _, yd, yu = copies(tag)
        pl.when(low_y)(yd.start)
        pl.when(high_y)(yu.start)

    def arrive(tag):
        xd, xu, yd, yu = copies(tag)
        pl.when(high_y)(yd.wait_recv)
        pl.when(low_y)(yu.wait_recv)
        pl.when(high_x)(xd.wait_recv)
        pl.when(low_x)(xu.wait_recv)

    def sent(tag):
        xd, xu, yd, yu = copies(tag)
        pl.when(low_x)(xd.wait_send)
        pl.when(high_x)(xu.wait_send)
        pl.when(low_y)(yd.wait_send)
        pl.when(high_y)(yu.wait_send)

    def unpack(tag):
        for x in range(nx):
            fields[tag][1 + x, pl.ds(PAD - 1, 1)] = yrecv[tag, 0, pl.ds(x, 1)]
            fields[tag][1 + x, pl.ds(PAD + ny, 1)] = yrecv[tag, 1, pl.ds(x, 1)]

    for load in loads:
        load.wait()

    for x in range(nx):
        at = pl.ds(x, 1)
        ysend[0, 0, at] = fields[0][x + 1, pl.ds(PAD, 1)]
        ysend[0, 1, at] = fields[0][x + 1, pl.ds(PAD + ny - 1, 1)]
        ysend[7, 1, at] = cy[x, pl.ds(PAD + ny - 1, 1)]
        ysend[8, 1, at] = py[x, pl.ds(ny - 1, 1)]
    dirs = [dirs_ref[d].astype(jnp.float32).T for d in range(3)]
    edge = jnp.broadcast_to(dirs_ref[1][:, ny - 1:], (nx, nz))
    ysend[8, 1] = jnp.where(edge > 0, ysend[8, 1], 0.0)

    def upper(d, x):
        column = (lax.broadcasted_iota(jnp.int32, (nx, nz), 0) == x).astype(jnp.float32)
        return jnp.dot(dirs[d], column, preferred_element_type=jnp.float32) > 0.5

    stage[...] = jnp.where(upper(0, nx - 1), px[nx - 1], 0.0)
    start_x(0)
    start_y(0)
    statics = (
        (x_up(7, cx.at[nx], landed.at[0]), y_up(7)),
        (x_up(8, stage, landed.at[1]), y_up(8)),
    )
    for xu, yu in statics:
        pl.when(high_x)(xu.start)
        pl.when(high_y)(yu.start)

    def masks(x, carry):
        low = [jnp.where(upper(d, x), ref[x], 0.0) for d, ref in enumerate((px, py, pz))]
        return carry, (low, [ref[x] - m for m, ref in zip(low, (px, py, pz))], cz[x])

    def store_masks(x, kept):
        low, high, c = kept
        mx[x + 1] = low[0]
        my[x, own] = low[1]
        mz[x] = jnp.where(last_lane, 0.0, low[2])
        px[x], py[x] = high[0], high[1]
        pz[x] = high[2]
        czm[x] = jnp.where(last_lane, 0.0, c)

    grouped("masks", 0, nx, masks, store_masks, 0)

    def diagonals(x, carry):
        p = pz[x]
        f = px[x] + mx[x] + py[x] + my[x, down] + p + behind_z(mz[x])
        g = cx[x + 1] + cx[x] + cy[x, own] + cy[x, down] + cz[x] + behind_z(czm[x])
        return carry, (f, g, jnp.where(last_lane, 0.0, p))

    def store_diagonals(x, kept):
        fdiag[x], gdiag[x], pz[x] = kept

    grouped("diagonals", 0, nx, diagonals, store_diagonals, 0)

    arrive(0)
    for xu, yu in statics:
        pl.when(low_x)(xu.wait_recv)
        pl.when(low_y)(yu.wait_recv)
    unpack(0)
    cx[0] = landed[0]
    mx[0] = landed[1]
    gdiag[0] += cx[0]
    fdiag[0] += mx[0]
    first = pl.ds(0, 1)
    for x in range(nx):
        row = yrecv[7, 0, pl.ds(x, 1)]
        cy[x, pl.ds(PAD - 1, 1)] = row
        gdiag[x, first] += row
        row = yrecv[8, 0, pl.ds(x, 1)]
        my[x, pl.ds(PAD - 1, 1)] = row
        fdiag[x, first] += row

    def spread(ref, x):
        v = ref[x + 1, own]
        total = cx[x + 1] * ref[x + 2, own] + cx[x] * ref[x, own]
        total += cy[x, own] * ref[x + 1, up] + cy[x, down] * ref[x + 1, down]
        c = czm[x]
        total += c * ahead_z(v) + behind_z(c * v)
        return v, total - gdiag[x] * v

    def carried(ref, x):
        v = ref[x + 1, own]
        total = px[x] * ref[x + 2, own] + mx[x] * ref[x, own]
        total += py[x] * ref[x + 1, up] + my[x, down] * ref[x + 1, down]
        total += pz[x] * ahead_z(v) + behind_z(mz[x] * v)
        return total - fdiag[x] * v

    def fold(v):
        return jnp.sum(v.reshape(v.shape[0] // 8, 8, nz), axis=0)

    nothing = jnp.zeros((8, nz), jnp.float32)

    def keep(tag, x, v):
        fields[tag][x + 1, own] = v
        ysend[tag, 0, pl.ds(x, 1)] = v[:1]
        ysend[tag, 1, pl.ds(x, 1)] = v[ny - 1:]

    def across(step, slots, axis, me, count, send, recv):
        out = [
            pltpu.make_async_remote_copy(
                slots.at[step, me], slots.at[step, me], send.at[step, off], recv.at[step, me],
                device_id={axis: lax.rem(me + off, count)}, device_id_type=MESH)
            for off in range(1, count)
        ]
        for copy in out:
            copy.start()

        def result():
            for off in range(1, count):
                peer = lax.rem(me + off, count)
                pltpu.make_async_remote_copy(
                    slots.at[step, peer], slots.at[step, peer], send.at[step, off], recv.at[step, peer],
                    device_id={axis: peer}, device_id_type=MESH).wait_recv()
            total = slots[step, 0]
            for k in range(1, count):
                total = total + slots[step, k]
            return total

        return out, result

    row_x = lax.broadcasted_iota(jnp.int32, (nx, nz), 0)
    between = jnp.logical_and(row_x > 0, row_x < nx - 1)
    pending = []
    for step, section in enumerate((3, 2, 1)):
        r_tag, w_tag = 1 + step, 4 + step
        r_ref, w_ref = fields[r_tag], fields[w_tag]

        def first_pass(x, m0):
            if step == 0:
                c_ref = fields[0]
                r = section_weights[3] * (spread(c_ref, x)[1] + carried(c_ref, x))
            else:
                r = following(x)
            r, more = r if step else (r, None)
            return m0 + fold(r * r), (r, more)

        def store_first(x, kept):
            r, more = kept
            keep(r_tag, x, r)
            if more is not None:
                fr[step - 1][x], dw[step - 1][x] = more

        m0 = nothing
        for x in (0, nx - 1):
            m0, kept = first_pass(x, m0)
            store_first(x, kept)
        start_x(r_tag)
        m0 = grouped("next" if step else "source", 1, nx - 1, first_pass, store_first, m0)
        start_y(r_tag)

        def second_pass(x, sums):
            m1, m2 = sums
            r, d = spread(r_ref, x)
            w = r - implicit_diagonal * d
            return (m1 + fold(r * w), m2 + fold(w * w)), w

        def store_second(x, w):
            keep(w_tag, x, w)

        sums = grouped("image", 1, nx - 1, second_pass, store_second, (nothing, nothing))
        arrive(r_tag)
        unpack(r_tag)
        for x in (0, nx - 1):
            sums, w = second_pass(x, sums)
            store_second(x, w)
        m1, m2 = sums
        start_x(w_tag)
        for side, face in ((0, yrecv[7, 0]), (1, ysend[7, 1])):
            change = jnp.where(between, -implicit_diagonal * face * yrecv[r_tag, side], 0.0)
            w = ysend[w_tag, side]
            ysend[w_tag, side] = w + change
            m1 += fold(ysend[r_tag, side] * change)
            m2 += fold((2.0 * w + change) * change)
        start_y(w_tag)
        for x in range(1, nx - 1):
            fields[w_tag][1 + x, pl.ds(PAD, 1)] = ysend[w_tag, 0, pl.ds(x, 1)]
            fields[w_tag][1 + x, pl.ds(PAD + ny - 1, 1)] = ysend[w_tag, 1, pl.ds(x, 1)]

        def third_pass(x, m3):
            w = w_ref[x + 1, own]
            jump_x = w_ref[x + 2, own] - w
            jump_y = w_ref[x + 1, up] - w
            jump_z = jnp.where(last_lane, 0.0, ahead_z(w)) - w
            total = cx[x + 1] * jump_x * jump_x + cy[x, own] * jump_y * jump_y
            total += cz[x] * jump_z * jump_z
            return m3 + fold(total), None

        m3 = grouped("energy", 0, nx - 1, third_pass, lambda x, kept: None, nothing)

        def store_r(x, kept):
            fr[step][x] = kept

        grouped("carry", 0, nx, lambda x, c: (c, carried(r_ref, x)), store_r, 0)
        arrive(w_tag)
        m3, _ = third_pass(nx - 1, m3)
        above = yrecv[w_tag, 1]
        m3 += fold(ysend[7, 1] * above * (above - 2.0 * ysend[w_tag, 1]))
        m3 = m2 + implicit_diagonal * m3
        rows = [jnp.sum(m, axis=0, keepdims=True) for m in (m0, m1, m2, m3)]
        red_y[step, me_y] = jnp.concatenate(rows + [jnp.zeros((4, nz), jnp.float32)], axis=0)
        out, result = across(step, red_y, "gy", me_y, gy, rys, ryr)
        pending += out
        unpack(w_tag)

        def store_w(x, kept):
            fw[step][x], dw[step][x] = kept

        grouped("both", 0, nx, lambda x, c: (c, (carried(w_ref, x), spread(w_ref, x)[1])), store_w, 0)
        red_x[step, me_x] = result()
        out, result = across(step, red_x, "gx", me_x, gx, rxs, rxr)
        pending += out

        target = section - 1
        share = section_weights[target] / section_weights[3]

        def gather(x, carry):
            total = share * fields[1][x + 1, own]
            for k in range(step):
                total += explicit_table[3 - k][target] * fr[k][x] + implicit_table[3 - k][target] * dw[k][x]
            if target == 0:
                total += fields[0][x + 1, own]
                for k in range(step):
                    on_r, on_w = weights[k]
                    total += on_r * fields[1 + k][x + 1, own] + on_w * fields[4 + k][x + 1, own]
            return carry, total

        if step == 0:
            weights = []
        def store_base(x, kept):
            base[x] = kept

        grouped("gather", 0, nx, gather, store_base, 0)

        total = result()
        total = jnp.broadcast_to(jnp.sum(total, axis=1, keepdims=True), (8, nz))
        m0, m1, m2, m3 = [total[k:k + 1] for k in range(4)]
        alpha = m0 / m1
        rr = alpha * alpha * m2 - m0
        ratio = rr / m0
        product = m1 - 2.0 * alpha * m2 + alpha * alpha * m3
        alpha_next = rr / (product - ratio * rr / alpha)
        on_r = alpha + alpha_next * (1.0 + ratio)
        on_w = -alpha_next * alpha
        weights.append((on_r, on_w))

        def following(x, step=step, section=section, target=target, on_r=on_r, on_w=on_w):
            r, w = fields[1 + step][x + 1, own], fields[4 + step][x + 1, own]
            advected = on_r * fr[step][x] + on_w * fw[step][x]
            diffused = (on_r / implicit_diagonal) * (r - w) + on_w * dw[step][x]
            total = base[x]
            total += explicit_table[section][target] * advected
            total += implicit_table[section][target] * diffused
            if target == 0:
                return total + on_r * r + on_w * w
            return total, (advected, diffused)

    def last(x, carry):
        out_ref[x] = following(x)
        return carry

    lax.fori_loop(0, nx, last, 0)
    for xu, yu in statics:
        pl.when(high_x)(xu.wait_send)
        pl.when(high_y)(yu.wait_send)
    for tag in range(7):
        sent(tag)
    for copy in pending:
        copy.wait_send()


def local(gx, gy, cotangent, speed, coeff, dirs):
    nx, ny, nz = cotangent.shape
    f32 = jnp.float32
    rows = ny + 2 * PAD
    plain = pltpu.VMEM((nx, ny, nz), f32)
    dma = pltpu.SemaphoreType.DMA
    anywhere = pl.BlockSpec(memory_space=pl.ANY)
    return pl.pallas_call(
        functools.partial(kernel, gx, gy),
        out_shape=jax.ShapeDtypeStruct((nx, ny, nz), f32),
        in_specs=[anywhere, anywhere, anywhere, pl.BlockSpec(memory_space=pltpu.VMEM)],
        out_specs=pl.BlockSpec(memory_space=pltpu.VMEM),
        scratch_shapes=[
            *[pltpu.VMEM((nx + 2, rows, nz), f32)] * 7,
            *[plain] * 9,
            plain,
            pltpu.VMEM((nx + 1, ny, nz), f32),
            pltpu.VMEM((nx, rows, nz), f32),
            plain, plain,
            plain, plain, plain,
            pltpu.VMEM((nx + 1, ny, nz), f32),
            pltpu.VMEM((nx, rows, nz), f32),
            plain,
            plain, plain,
            pltpu.VMEM((9, 2, nx, nz), f32),
            pltpu.VMEM((9, 2, nx, nz), f32),
            pltpu.VMEM((2, ny, nz), f32),
            pltpu.VMEM((ny, nz), f32),
            pltpu.VMEM((3, gy, 8, nz), f32),
            pltpu.VMEM((3, gx, 8, nz), f32),
            dma((7,)), dma((9, 4)), dma((9, 4)),
            dma((3, gy)), dma((3, gy)), dma((3, gx)), dma((3, gx)),
        ],
        compiler_params=pltpu.CompilerParams(
            collective_id=0, has_side_effects=True, vmem_limit_bytes=60 * 1024 * 1024
        ),
    )(cotangent, speed, coeff, dirs)


def solution(mesh):
    return jax.shard_map(
        functools.partial(local, mesh.shape["gx"], mesh.shape["gy"]),
        mesh=mesh,
        in_specs=(
            P("gx", "gy", None),
            P(None, "gx", "gy", None),
            P(None, "gx", "gy", None),
            P(None, "gx", "gy"),
        ),
        out_specs=P("gx", "gy", None),
        check_vma=False,
    )
```
